32 devices in a mesh: section: 2 (over x), expert: 4 (over y, core), dp: 4 (over z).
Axes of the slice: x: 2, y: 2, z: 4, core: 2. Of those that a mesh axis runs over, the one named last changes fastest.
Arguments:
- x_in: bfloat16 [8, 256, 2048], P(None, ('expert', 'dp'), 'section'), may hold values from -6 to 6
- cotangent: bfloat16 [8, 256, 2048], P(None, ('expert', 'dp'), 'section'), may hold values from -6 to 6
- route_ids: int32 [2, 8, 256, 2], P('section', None, ('expert', 'dp')), may hold values from 0 to 15, all different within a row; in each aligned block of 16 rows (0 to 15, 16 to 31, ..., all dimensions but the last counted through in order) at most 2 rows name the same one
- norm_gain: float32 [2, 2048], P('section'), may hold values from 0.5 to 1.5
- router: bfloat16 [2, 2048, 16], P('section'), may hold values from -0.125 to 0.125
- w_gate_up: bfloat16 [2, 16, 2048, 1024], P('section', ('expert', 'dp')), may hold values from -0.125 to 0.125
- w_down: bfloat16 [2, 16, 512, 2048], P('section', ('expert', 'dp')), may hold values from -0.25 to 0.25
Outputs:
- grad_in: bfloat16 [8, 256, 2048], P(None, ('expert', 'dp'), 'section')
- grad_gate_up: float32 [2, 16, 2048, 1024], P('section', ('expert', 'dp'))
- grad_down: float32 [2, 16, 512, 2048], P('section', ('expert', 'dp'))
- grad_router: float32 [2, 2048, 16], P('section')
- grad_gain: float32 [2, 2048], P('section')
The draws below stay inside these ranges and needn't reach their ends.
Inputs may be any that keep to these rules, and one draw needn't show every extreme that they name: `route_ids`: each row names two different experts; the 16 rows of one device in one layer and micro-batch name any expert at most 2 times, a bound that some block reaches in some of them.
All inputs are finite; a program needn't handle non-finite values.
Results may differ from the reference program's by a relative error of at most 0.035.
Values may be sent and summed in bfloat16 or wider, within the bound.
A program may use at most 64 MiB of HBM per device.

```python
import math
import jax
import jax.numpy as jnp
import numpy as np
from jax import lax

D = 2048
FFW = 512
TOP = 2
MICRO = 8
TOK_DEV = 16
EXPERTS = 16
CAP = 2
ROWS = 256
SECTIONS = 2


def shard_levels(own_key, shape, pieces, low, high):
    def one(axis_at, blocks):
        heights = jax.random.uniform(jax.random.fold_in(jax.random.fold_in(own_key, 6), axis_at), (blocks,), jnp.float32, low / len(pieces), high / len(pieces))
        return jnp.repeat(jnp.exp(heights), shape[axis_at] // blocks).reshape((-1,) + (1,) * (len(shape) - axis_at - 1))

    level = one(*pieces[0])
    for cut in pieces[1:]:
        level = level * one(*cut)
    return level


def routed_block(key, own, number, rows, count, top, reach, lean):
    sequence = jax.random.permutation(key, count)
    packed, ordinary = shares(count, rows * top, reach, lean, True), shares(count, rows * top, reach, lean, False)
    places = jnp.arange(count)

    def named(lengths, turn):
        used = int((lengths > 0).sum())
        fixed = max(1, used // 4)
        moved = fixed + (places - fixed + turn * (used - fixed)) % max(1, count - fixed)
        return jnp.zeros((count,), jnp.int32).at[sequence[jnp.where(places < fixed, places, moved)]].set(jnp.asarray(lengths, jnp.int32))

    lengths = jnp.where(number % 4 == 0, named(packed, number // 4), named(ordinary, number - number // 4 - 1))
    mixed = jax.random.permutation(jax.random.fold_in(own, 3), count)
    donor, taker = mixed[0:count // 2 * 2:2], mixed[1:count // 2 * 2:2]
    slack = jnp.minimum(lengths[donor] - 1, reach - lengths[taker]) // 2
    slack = jnp.where((donor == sequence[0]) | (taker == sequence[0]) | (lengths[taker] == 0), 0, jnp.maximum(slack, 0))
    moved = jax.random.randint(jax.random.fold_in(own, 4), (count // 2,), 0, 1 << 20) % (slack + 1)
    lengths = lengths.at[donor].add(-moved).at[taker].add(moved)
    items = jnp.searchsorted(jnp.cumsum(lengths), jnp.arange(rows * top), side="right").astype(jnp.int32)
    listing = items.reshape(top, rows).T
    listing = listing[jax.random.permutation(jax.random.fold_in(own, 1), rows)]
    turn = jax.random.randint(jax.random.fold_in(own, 2), (rows, 1), 0, top)
    return jnp.take_along_axis(listing, (jnp.arange(top)[None, :] + turn) % top, axis=1)


def shares(count, total, bound, slope, full):
    portions = [(1 << 20) // math.isqrt(rank ** slope) + 1 for rank in range(1, count + 1)]
    largest = bound if full else min(bound, max(-(-total // count), total * portions[0] // sum(portions)))
    least = 1 if total - largest >= count - 1 else 0
    holding, rest = [largest] + [least] * (count - 1), total - largest - least * (count - 1)
    while rest > 0:
        candidates = [i for i in range(1, count) if holding[i] < largest] or [i for i in range(1, count) if holding[i] < bound]
        mass, budget = sum([portions[i] for i in candidates]), rest
        for i in candidates:
            addition = min(bound - holding[i], max(1, budget * portions[i] // mass), rest)
            holding[i] = holding[i] + addition
            rest = rest - addition
    return np.array(holding)


def gaussian(stream_key, dims, width, limit, shards=(), kind=jnp.bfloat16):
    array = jax.random.normal(stream_key, dims, jnp.float32) * width
    if len(shards) > 0:
        array = shard_levels(stream_key, dims, shards, -0.22, 0.18) * array
    return jnp.clip(array, min=-limit, max=limit).astype(kind)


def setup_inputs(seed: int = 0) -> dict:
    arg_keys = jax.random.split(jax.random.key(seed), 8)
    x_in = gaussian(arg_keys[0], (MICRO, ROWS, D), 1.0, 6.0, ((1, 16), (2, 2)))
    cotangent = gaussian(arg_keys[1], (MICRO, ROWS, D), 1.0, 6.0, ((1, 16), (2, 2)))
    route_ids_keys = jax.random.split(jax.random.fold_in(arg_keys[2], 1), SECTIONS * MICRO * ROWS // TOK_DEV)
    route_ids_turns = jax.random.permutation(jax.random.fold_in(arg_keys[2], 3), SECTIONS * MICRO * ROWS // TOK_DEV)
    route_ids = jax.vmap(lambda own, number: routed_block(jax.random.fold_in(arg_keys[2], 2), own, number, TOK_DEV, EXPERTS, TOP, CAP, 2))(route_ids_keys, route_ids_turns).reshape((SECTIONS, MICRO, ROWS, TOP))
    norm_gain = jnp.clip(1.0 + 0.1 * jax.random.normal(arg_keys[3], (SECTIONS, D), jnp.float32), 0.5, 1.5)
    router = gaussian(arg_keys[4], (SECTIONS, D, EXPERTS), D ** -0.5, 0.125, ((0, 2),))
    w_gate_up = gaussian(arg_keys[5], (SECTIONS, EXPERTS, D, 2 * FFW), D ** -0.5, 0.125, ((0, 2), (1, 16)))
    w_down = gaussian(arg_keys[6], (SECTIONS, EXPERTS, FFW, D), FFW ** -0.5, 0.25, ((0, 2), (1, 16)))
    return dict(x_in=x_in, cotangent=cotangent, route_ids=route_ids, norm_gain=norm_gain, router=router, w_gate_up=w_gate_up, w_down=w_down)


EPS = 1e-05

def rounded(value):
    return lax.optimization_barrier(value.astype(jnp.bfloat16))

def slot_tables(route_rows):
    experts = jnp.arange(EXPERTS, dtype=jnp.int32)
    expert_hits = (route_rows[..., None] == experts).astype(jnp.int32)
    per_expert = lax.optimization_barrier(jnp.sum(expert_hits, axis=-2))
    before = jnp.cumsum(per_expert, axis=-2) - per_expert
    slot_ids = lax.optimization_barrier(jnp.sum(expert_hits * before[..., None, :], axis=-1))
    dest_cell = route_rows * CAP + slot_ids
    cell_ids = jnp.arange(EXPERTS * CAP, dtype=jnp.int32)
    slot_place = (dest_cell[..., None] == cell_ids).astype(jnp.float32)
    return (expert_hits.astype(jnp.float32), slot_place)

def layer_state(layer_in, route_rows, gain_vec, router_mat, w_gu):
    blocks = ROWS // TOK_DEV
    h_wide = layer_in.reshape(MICRO, blocks, TOK_DEV, D).astype(jnp.float32)
    inv_rms = lax.rsqrt(lax.optimization_barrier(jnp.mean(h_wide * h_wide, axis=-1, keepdims=True)) + EPS)
    normed = rounded(h_wide * inv_rms * gain_vec).astype(jnp.float32)
    expert_hits, slot_place = slot_tables(route_rows.reshape(MICRO, blocks, TOK_DEV, TOP))
    logits = jnp.einsum('mbtd,de->mbte', normed, router_mat.astype(jnp.float32), precision=lax.Precision.HIGHEST)
    chosen = lax.optimization_barrier(jnp.sum(expert_hits * logits[..., None, :], axis=-1))
    first_gate = jax.nn.sigmoid(chosen[..., 0] - chosen[..., 1])
    second_gate = jax.nn.sigmoid(chosen[..., 1] - chosen[..., 0])
    exp_rows = rounded(jnp.einsum('mbtkc,mbtd->mbcd', slot_place, normed, precision=lax.Precision.HIGHEST))
    exp_rows = exp_rows.astype(jnp.float32).reshape(MICRO, blocks, EXPERTS, CAP, D)
    gate_up = jnp.einsum('mbecd,edf->mbecf', exp_rows, w_gu.astype(jnp.float32), precision=lax.Precision.HIGHEST)
    gate_part = gate_up[..., :FFW]
    up_part = gate_up[..., FFW:]
    sigmoid_gate = jax.nn.sigmoid(gate_part)
    hidden = rounded(gate_part * sigmoid_gate * up_part).astype(jnp.float32)
    return (h_wide, inv_rms, normed, expert_hits, slot_place, first_gate, second_gate, exp_rows, gate_part, up_part, sigmoid_gate, hidden)

def expert_out(hidden, w_dn):
    blocks = ROWS // TOK_DEV
    out_rows = rounded(jnp.einsum('mbecf,efd->mbecd', hidden, w_dn.astype(jnp.float32), precision=lax.Precision.HIGHEST))
    return out_rows.astype(jnp.float32).reshape(MICRO, blocks, EXPERTS * CAP, D)

def forward_layer(layer_in, route_rows, gain_vec, router_mat, w_gu, w_dn):
    state = layer_state(layer_in, route_rows, gain_vec, router_mat, w_gu)
    h_wide, slot_place, first_gate, second_gate, hidden = (state[0], state[4], state[5], state[6], state[11])
    picked = jnp.einsum('mbtkc,mbcd->mbtkd', slot_place, expert_out(hidden, w_dn), precision=lax.Precision.HIGHEST)
    layer_out = h_wide + first_gate[..., None] * picked[..., 0, :] + second_gate[..., None] * picked[..., 1, :]
    return layer_out.astype(jnp.bfloat16).reshape(MICRO, ROWS, D)

def backward_layer(layer_in, grad_top, route_rows, gain_vec, router_mat, w_gu, w_dn):
    blocks = ROWS // TOK_DEV
    h_wide, inv_rms, normed, expert_hits, slot_place, first_gate, second_gate, exp_rows, gate_part, up_part, sigmoid_gate, hidden = layer_state(layer_in, route_rows, gain_vec, router_mat, w_gu)
    grad_wide = grad_top.reshape(MICRO, blocks, TOK_DEV, D).astype(jnp.float32)
    gates = jnp.stack([first_gate, second_gate], axis=-1)
    scaled = rounded(gates[..., None] * grad_wide[..., None, :]).astype(jnp.float32)
    dy_rows = rounded(jnp.einsum('mbtkc,mbtkd->mbcd', slot_place, scaled, precision=lax.Precision.HIGHEST))
    dy_rows = dy_rows.astype(jnp.float32).reshape(MICRO, blocks, EXPERTS, CAP, D)
    d_hidden = jnp.einsum('mbecd,efd->mbecf', dy_rows, w_dn.astype(jnp.float32), precision=lax.Precision.HIGHEST)
    silu_gate = gate_part * sigmoid_gate
    silu_slope = sigmoid_gate * (1.0 + gate_part * (1.0 - sigmoid_gate))
    gate_up_grad = rounded(jnp.concatenate([d_hidden * up_part * silu_slope, d_hidden * silu_gate], axis=-1))
    gate_up_grad = gate_up_grad.astype(jnp.float32)
    rows_grad = rounded(jnp.einsum('mbecf,edf->mbecd', gate_up_grad, w_gu.astype(jnp.float32), precision=lax.Precision.HIGHEST))
    rows_grad = rows_grad.astype(jnp.float32).reshape(MICRO, blocks, EXPERTS * CAP, D)
    grad_gu = jnp.einsum('mbecd,mbecf->edf', exp_rows, gate_up_grad, precision=lax.Precision.HIGHEST)
    grad_dn = jnp.einsum('mbecf,mbecd->efd', hidden, dy_rows, precision=lax.Precision.HIGHEST)
    normed_grad = jnp.einsum('mbtkc,mbcd->mbtd', slot_place, rows_grad, precision=lax.Precision.HIGHEST)
    picked = jnp.einsum('mbtkc,mbcd->mbtkd', slot_place, expert_out(hidden, w_dn), precision=lax.Precision.HIGHEST)
    gate_grad = lax.optimization_barrier(jnp.sum(grad_wide[..., None, :] * picked, axis=-1))
    logit_grad = first_gate * second_gate * (gate_grad[..., 0] - gate_grad[..., 1])
    logit_cols = logit_grad[..., None] * (expert_hits[..., 0, :] - expert_hits[..., 1, :])
    normed_grad = normed_grad + jnp.einsum('mbte,de->mbtd', logit_cols, router_mat.astype(jnp.float32), precision=lax.Precision.HIGHEST)
    grad_rt = jnp.einsum('mbtd,mbte->de', normed, logit_cols, precision=lax.Precision.HIGHEST)
    grad_gn = lax.optimization_barrier(jnp.sum(normed_grad * h_wide * inv_rms, axis=(0, 1, 2)))
    scaled_grad = normed_grad * gain_vec
    projection = lax.optimization_barrier(jnp.mean(scaled_grad * h_wide, axis=-1, keepdims=True))
    input_grad = grad_wide + inv_rms * scaled_grad - h_wide * inv_rms * inv_rms * inv_rms * projection
    return (input_grad.astype(jnp.bfloat16).reshape(MICRO, ROWS, D), (grad_gu, grad_dn, grad_rt, grad_gn))

def reference(x_in, cotangent, route_ids, norm_gain, router, w_gate_up, w_down):

    def forward_step(layer_in, params):
        route_rows, gain_vec, router_mat, w_gu, w_dn = params
        return (forward_layer(layer_in, route_rows, gain_vec, router_mat, w_gu, w_dn), layer_in)
    _, inputs = lax.scan(forward_step, x_in, (route_ids, norm_gain, router, w_gate_up, w_down))

    def backward_step(grad_top, params):
        route_rows, gain_vec, router_mat, w_gu, w_dn, layer_in = params
        return backward_layer(layer_in, grad_top, route_rows, gain_vec, router_mat, w_gu, w_dn)
    grad_in, grad_list = lax.scan(backward_step, cotangent, (route_ids, norm_gain, router, w_gate_up, w_down, inputs), reverse=True)
    return (grad_in, grad_list[0], grad_list[1], grad_list[2], grad_list[3])
```

```python
import functools

import jax
import jax.numpy as jnp
from jax import lax
from jax.experimental import pallas as pl
from jax.experimental.pallas import tpu as pltpu
from jax.sharding import PartitionSpec as P

EPS = 1e-05
CHUNKS = 2
LANES = 128
F32 = jnp.float32
BF16 = jnp.bfloat16


def exchange_body(n_arr, n_expert_axis, n_dp_axis, *refs):
    ins, outs = refs[:n_arr], refs[n_arr : 2 * n_arr]
    send_sem, recv_sem = refs[2 * n_arr :]
    n_rank = n_expert_axis * n_dp_axis
    me = lax.axis_index("expert") * n_dp_axis + lax.axis_index("dp")

    def place(step):
        rank = lax.rem(me + step, n_rank)
        return rank, {"expert": lax.div(rank, n_dp_axis), "dp": lax.rem(rank, n_dp_axis)}

    barrier = pltpu.get_barrier_semaphore()
    for step in range(1, n_rank):
        pl.semaphore_signal(
            barrier, inc=1, device_id=place(step)[1], device_id_type=pl.DeviceIdType.MESH
        )
    pl.semaphore_wait(barrier, n_rank - 1)
    copies = []
    for step in range(1, n_rank):
        rank, device = place(step)
        for i in range(n_arr):
            copy = pltpu.make_async_remote_copy(
                src_ref=ins[i].at[rank],
                dst_ref=outs[i].at[me],
                send_sem=send_sem.at[i, step],
                recv_sem=recv_sem.at[i, step],
                device_id=device,
                device_id_type=pl.DeviceIdType.MESH,
            )
            copy.start()
            copies.append(copy)
    for i in range(n_arr):
        outs[i][me] = ins[i][me]
    for copy in copies:
        copy.wait()


def exchange(arrays, collective_id):
    n_rank = arrays[0].shape[0]
    n_expert_axis, n_dp_axis = lax.axis_size("expert"), lax.axis_size("dp")
    spec = pl.BlockSpec(memory_space=pltpu.VMEM)
    return pl.pallas_call(
        functools.partial(exchange_body, len(arrays), n_expert_axis, n_dp_axis),
        out_shape=[jax.ShapeDtypeStruct(a.shape, a.dtype) for a in arrays],
        in_specs=[spec] * len(arrays),
        out_specs=[spec] * len(arrays),
        scratch_shapes=[
            pltpu.SemaphoreType.DMA((len(arrays), n_rank)),
            pltpu.SemaphoreType.DMA((len(arrays), n_rank)),
        ],
        compiler_params=pltpu.CompilerParams(
            collective_id=collective_id, has_side_effects=True
        ),
    )(*arrays)


def dot(a, b, dims, precision=None):
    return lax.dot_general(
        a, b, ((dims[:1], dims[1:]), ((), ())), precision=precision, preferred_element_type=F32
    )


def place_tables(route_all, n_expert, capacity, chunks):
    micro, tok, _ = route_all.shape
    per = micro // chunks
    hits = (route_all[..., None] == jnp.arange(n_expert, dtype=jnp.int32)).astype(jnp.int32)
    named = jnp.sum(hits, axis=2)
    earlier = (jnp.arange(tok)[:, None] > jnp.arange(tok)[None, :]).astype(jnp.int32)
    before = jnp.sum(earlier[None, :, :, None] * named[:, None, :, :], axis=2)
    slot = jnp.sum(hits * before[:, :, None, :], axis=3)
    within = (jnp.arange(micro, dtype=jnp.int32) % per)[:, None, None]
    cell = route_all * (per * capacity) + within * capacity + slot
    cell = jnp.transpose(cell.reshape(chunks, per * tok, 2), (0, 2, 1))
    cells = jnp.arange(n_expert * per * capacity, dtype=jnp.int32)
    tables = (cell[:, :, None, :] == cells[None, None, :, None]).astype(BF16)
    return tables, hits.reshape(chunks, per * tok, 2, n_expert).astype(F32)


def pick(stack, index):
    return lax.dynamic_index_in_dim(stack, index, 0, keepdims=False)


def keep(stack, index, value, active):
    return lax.dynamic_update_index_in_dim(
        stack, jnp.where(active, value, pick(stack, index)), index, 0
    )


def ends_gather(x_in, cotangent, section, n_section):
    if n_section == 1:
        return x_in, cotangent
    x_parts, top_parts = [], []
    last = n_section - 1
    for source in range(n_section):
        if source == 0:
            x_parts.append(x_in)
            continue
        other = last - source
        if other != source:
            got = lax.ppermute(
                jnp.where(section == source, x_in, cotangent),
                "section",
                [(source, 0), (other, last)],
            )
            x_parts.append(got)
            top_parts.append(got)
        else:
            x_parts.append(lax.ppermute(x_in, "section", [(source, 0)]))
            top_parts.append(lax.ppermute(cotangent, "section", [(other, last)]))
    top_parts = top_parts[::-1] + [cotangent]
    return jnp.concatenate(x_parts, axis=2), jnp.concatenate(top_parts, axis=2)


def local(x_in, cotangent, route_ids, norm_gain, router, w_gate_up, w_down):
    micro, tok, _ = x_in.shape
    n_section = lax.axis_size("section")
    n_rank = lax.axis_size("expert") * lax.axis_size("dp")
    per_rank, hidden_width, width = w_down.shape[1:]
    assert per_rank == 1
    n_expert = n_rank
    capacity = tok * 2 * 9 // (8 * n_expert)
    section = lax.axis_index("section")
    last = n_section - 1
    chunks = CHUNKS if n_section > 1 and micro % CHUNKS == 0 else 1
    per = micro // chunks
    tokens = per * tok
    block = per * capacity
    cells = n_rank * block
    gain = norm_gain[0]
    router_mat = router[0]
    router_wide = router_mat.astype(F32)
    w_gu, w_dn = w_gate_up[0, 0], w_down[0, 0]

    x_all, top_all = ends_gather(x_in, cotangent, section, n_section)
    x_all = x_all.reshape(chunks, tokens, width)
    top_all = top_all.reshape(chunks, tokens, width)
    tables, hits_all = place_tables(route_ids[0], n_expert, capacity, chunks)

    zero_rows = jnp.zeros((chunks, cells, width), BF16)
    stash_h = jnp.zeros((chunks, tokens, width), BF16)
    stash_rows, stash_top, stash_dy = zero_rows, zero_rows, zero_rows
    stash_gate = jnp.zeros((chunks, cells), F32)
    stash_hidden = jnp.zeros((chunks, cells, hidden_width), BF16)
    stash_q = jnp.zeros((chunks, cells, 2 * hidden_width), BF16)
    stash_out = jnp.zeros((chunks, tokens, width), BF16)
    acc_router = jnp.zeros((n_expert, width), F32)
    acc_gain = jnp.zeros((width,), F32)
    got_h = jnp.zeros((tokens, width), BF16)
    got_g = jnp.zeros((tokens, width), BF16)

    def both(index):
        return pick(tables, index)[0] + pick(tables, index)[1]

    def blocks(rows):
        return rows.reshape(n_rank, block, rows.shape[-1])

    def lanes(column):
        return jnp.broadcast_to(column[:, None], (cells, LANES)).reshape(n_rank, block, LANES)

    if n_section == 1:
        rows = [blocks(dot(both(c), top_all[c], (1, 0)).astype(BF16)) for c in range(chunks)]
        for c in range(chunks):
            got, _ = exchange([rows[c], lanes(jnp.zeros((cells,), F32))], 0)
            stash_top = stash_top.at[c].set(got.reshape(cells, width))

    for tick in range(chunks + 2 * last):
        any_f = any(0 <= tick - s < chunks for s in range(last))
        any_t = 0 <= tick - last < chunks
        any_b = any(0 <= tick - 2 * last + s < chunks for s in range(last))
        up, down = tick - section, tick - 2 * last + section
        is_top = section == last
        is_f = (up >= 0) & (up < chunks) & ~is_top
        is_t = (up >= 0) & (up < chunks) & is_top
        is_b = (down >= 0) & (down < chunks) & ~is_top
        seed = tick == 0 and n_section > 1
        index = jnp.clip(jnp.where(is_b, down, up), 0, chunks - 1)

        h = got_h
        if tick < chunks:
            h = jnp.where(section == 0, pick(x_all, index), h)
        if any_b:
            h = jnp.where(is_b, pick(stash_h, index), h)
        h_wide = h.astype(F32)
        inv = lax.rsqrt(jnp.mean(h_wide * h_wide, axis=-1, keepdims=True) + EPS)
        u = (h_wide * inv * gain).astype(BF16)
        hits = pick(hits_all, index)
        logits = dot(u, router_mat, (1, 0))
        chosen = jnp.sum(hits * logits[:, None, :], axis=2)
        gate_1 = jax.nn.sigmoid(chosen[:, 0] - chosen[:, 1])
        gate_2 = jax.nn.sigmoid(chosen[:, 1] - chosen[:, 0])
        pair = pick(tables, index)
        first, second = pair[0], pair[1]
        gate_cells = jnp.sum(
            first.astype(F32) * gate_1[None, :] + second.astype(F32) * gate_2[None, :], axis=1
        )
        if any_f or any_t:
            stash_h = keep(stash_h, index, h, is_f | is_t)
        g_top = got_g
        if any_t:
            g_top = jnp.where(is_t, pick(top_all, index), g_top)
        source = u
        if any_b:
            source = jnp.where(is_b, g_top, source) if any_t or any_f else g_top
        if seed:
            source = jnp.where(is_top, top_all[0], source)
        sent = dot(first + second, source, (1, 0)).astype(BF16)
        landed, side = exchange([blocks(sent), lanes(gate_cells)], 0)
        landed = landed.reshape(cells, width)
        gate_here = side.reshape(cells, LANES)[:, 0]
        if seed:
            stash_top = stash_top.at[0].set(jnp.where(is_top, landed, stash_top[0]))
        if any_f or any_t:
            stash_rows = keep(stash_rows, index, landed, is_f | is_t)
            stash_gate = keep(stash_gate, index, gate_here, is_f | is_t)
        if any_b:
            stash_top = keep(stash_top, index, landed, is_b)
        rows, gate_here = pick(stash_rows, index), pick(stash_gate, index)

        gate_up = dot(rows, w_gu, (1, 0))
        a, b = gate_up[:, :hidden_width], gate_up[:, hidden_width:]
        sig = jax.nn.sigmoid(a)
        hidden = (a * sig * b).astype(BF16)
        side_back = jnp.zeros((cells,), F32)
        if any_f:
            y = dot(hidden, w_dn, (1, 0)).astype(BF16)
            reply = y
        if any_t or any_b:
            top_rows = pick(stash_top, index)
            plain = dot(top_rows, w_dn, (1, 1))
            side_back = jnp.sum(plain * hidden.astype(F32), axis=1)
            d_hidden = plain * gate_here[:, None]
            slope = sig * (1.0 + a * (1.0 - sig))
            q = jnp.concatenate([d_hidden * b * slope, d_hidden * (a * sig)], axis=1).astype(BF16)
            dy = (top_rows.astype(F32) * gate_here[:, None]).astype(BF16)
            du_rows = dot(q, w_gu, (1, 1)).astype(BF16)
            stash_q = keep(stash_q, index, q, is_t | is_b)
            stash_dy = keep(stash_dy, index, dy, is_t | is_b)
            stash_hidden = keep(stash_hidden, index, hidden, is_t | is_b)
            reply = jnp.where(is_f, y, du_rows) if any_f else du_rows
        if seed and chunks > 1:
            later = dot(tables[1, 0] + tables[1, 1], top_all[1], (1, 0)).astype(BF16)
            reply = jnp.where(is_top, later, reply)
        back, side = exchange([blocks(reply), lanes(side_back)], 0)
        back = back.reshape(cells, width)
        if seed and chunks > 1:
            stash_top = stash_top.at[1].set(jnp.where(is_top, back, stash_top[1]))
        picked_1 = dot(first, back, (0, 0))
        picked_2 = dot(second, back, (0, 0))
        if any_f:
            h_next = (h_wide + gate_1[:, None] * picked_1 + gate_2[:, None] * picked_2).astype(BF16)
            got_h = lax.ppermute(h_next, "section", [(s, s + 1) for s in range(last)])
        if any_t or any_b:
            c_cells = side.reshape(cells, LANES)[:, :1]
            c_1 = jnp.sum(first.astype(F32) * c_cells, axis=0)
            c_2 = jnp.sum(second.astype(F32) * c_cells, axis=0)
            slope_l = gate_1 * gate_2 * (c_1 - c_2)
            cols = slope_l[:, None] * (hits[:, 0, :] - hits[:, 1, :])
            du = picked_1 + picked_2 + dot(cols, router_wide, (1, 1), lax.Precision.HIGHEST)
            mine = is_t | is_b
            term = dot(cols, u.astype(F32), (0, 0), lax.Precision.HIGHEST)
            acc_router = acc_router + jnp.where(mine, term, 0.0)
            acc_gain = acc_gain + jnp.where(mine, jnp.sum(du * h_wide * inv, axis=0), 0.0)
            scaled = du * gain
            projection = jnp.mean(scaled * h_wide, axis=-1, keepdims=True)
            g_out = (
                g_top.astype(F32) + inv * scaled - h_wide * (inv * inv * inv) * projection
            ).astype(BF16)
            stash_out = keep(stash_out, index, g_out, mine)
            if last > 0 and tick < chunks + 2 * last - 1:
                got_g = lax.ppermute(g_out, "section", [(s, s - 1) for s in range(1, n_section)])

    all_rows = stash_rows.reshape(chunks * cells, width)
    grad_gu = dot(all_rows, stash_q.reshape(chunks * cells, 2 * hidden_width), (0, 0))
    grad_dn = dot(
        stash_hidden.reshape(chunks * cells, hidden_width),
        stash_dy.reshape(chunks * cells, width),
        (0, 0),
    )

    high = -(-(n_expert + 1) // 8) * 8
    piece = width // n_rank
    acc = jnp.concatenate(
        [acc_router, acc_gain[None], jnp.zeros((high - n_expert - 1, width), F32)], axis=0
    )
    parts = jnp.transpose(acc.reshape(high, n_rank, piece), (1, 0, 2))
    (parts,) = exchange([parts], 1)
    total = jnp.broadcast_to(jnp.sum(parts, axis=0)[None], parts.shape)
    (total,) = exchange([total], 1)
    total = jnp.transpose(total, (1, 0, 2)).reshape(high, width)
    grad_router, grad_gain = total[:n_expert].T, total[n_expert]

    out = stash_out.reshape(micro, tok, n_section, width // n_section)
    grad_in = out[:, :, 0]
    for s in range(1, n_section):
        moved = lax.ppermute(out[:, :, s], "section", [(0, s)])
        grad_in = jnp.where(section == s, moved, grad_in)
    return (grad_in, grad_gu[None, None], grad_dn[None, None], grad_router[None], grad_gain[None])


def solution(mesh):
    in_specs = (
        P(None, ("expert", "dp"), "section"),
        P(None, ("expert", "dp"), "section"),
        P("section", None, ("expert", "dp"), None),
        P("section", None),
        P("section", None, None),
        P("section", ("expert", "dp"), None, None),
        P("section", ("expert", "dp"), None, None),
    )
    out_specs = (
        P(None, ("expert", "dp"), "section"),
        P("section", ("expert", "dp"), None, None),
        P("section", ("expert", "dp"), None, None),
        P("section", None, None),
        P("section", None),
    )
    return jax.shard_map(local, mesh=mesh, in_specs=in_specs, out_specs=out_specs, check_vma=False)
```
